32 devices in a mesh: grp: 16 (over z, x, core), tp: 2 (over y).
Axes of the slice: x: 2, y: 2, z: 4, core: 2. Of those that a mesh axis runs over, the one named last changes fastest.
Arguments:
- memory_rows: bfloat16 [16384, 4096], P('grp', 'tp'), may hold values from -24 to 24, as said below
- norm_gain: float32 [4096], replicated, may hold values from 0.25 to 1.75
- key_weight: bfloat16 [4096, 4096], P(None, 'tp'), may hold values from -0.09375 to 0.09375
- owner_table: int32 [2048], replicated, may hold values from 0 to 2047, as said below
Outputs:
- placed_keys: bfloat16 [16384, 4096], P('grp', 'tp')
The draws below stay inside these ranges and needn't reach their ends.
Inputs may be any that keep to these rules, and one draw needn't show every extreme that they name: A permutation of the 2048 block numbers. Block b of the input goes to block position owner_table[b], which lies in group owner_table[b] // 128. The 128 blocks of one group go to all 16 groups, exactly 8 blocks to each of them. `memory_rows`: rows have offsets and scales of their own, and features a common pattern.
All inputs are finite; a program needn't handle non-finite values.
Results may differ from the reference program's by a relative error of at most 0.0049.
Values may be sent and summed in bfloat16 or wider, within the bound.
A program may use at most 64 MiB of HBM per device.

```python
import jax
import jax.numpy as jnp
from jax import lax

D = 4096
BLK_ROWS = 8
BLK_DEV = 128
ROWS = 16384
NB = 2048


def draw_memory_rows(key, part):
    key_off, key_scale, key_noise, key_pattern = jax.random.split(key, 4)
    offsets = jax.random.uniform(key_off, (ROWS, 1), jnp.float32, -1.5, 1.5)
    pattern = jnp.clip(jax.random.normal(key_pattern, (1, D), jnp.float32), -3.0, 3.0)
    scales = jnp.exp(jax.random.uniform(key_scale, (ROWS, 1), jnp.float32, jnp.log(0.5), jnp.log(3.0)))
    noise = jnp.clip(jax.random.normal(key_noise, (ROWS, D), jnp.float32), -4.0, 4.0)
    values = offsets + scales * (noise + 0.7 * pattern)
    return jnp.clip(values, -24.0, 24.0).astype(jnp.bfloat16)


def draw_owner_table(key, part):
    groups = NB // BLK_DEV
    per_pair = BLK_DEV // groups
    key_tau, key_offs, key_cols, key_slots = jax.random.split(key, 4)
    shuffle = jax.random.permutation(key_tau, groups).astype(jnp.int32)
    offsets = jax.random.permutation(key_offs, groups).astype(jnp.int32)
    column_keys = jax.random.split(key_cols, groups)
    column_perm = jax.vmap(lambda one_key: jax.random.permutation(one_key, BLK_DEV))(column_keys).astype(jnp.int32)
    sources = jnp.arange(groups, dtype=jnp.int32)[:, None]
    target = shuffle[(sources + offsets[column_perm % groups]) % groups]
    arrival = sources * per_pair + column_perm // groups
    slot_keys = jax.random.split(key_slots, groups)
    slot_perm = jax.vmap(lambda one_key: jax.random.permutation(one_key, BLK_DEV))(slot_keys).astype(jnp.int32)
    slots = slot_perm[target, arrival]
    return (target * BLK_DEV + slots).reshape(-1).astype(jnp.int32)


def level_of(own_key, extent, cuts, low, high):
    def one(axis_at, blocks):
        draws = jax.random.uniform(jax.random.fold_in(jax.random.fold_in(own_key, 6), axis_at), (blocks,), jnp.float32, low / len(cuts), high / len(cuts))
        return jnp.repeat(jnp.exp(draws), extent[axis_at] // blocks).reshape((-1,) + (1,) * (len(extent) - axis_at - 1))

    factor_of = one(*cuts[0])
    for cut in cuts[1:]:
        factor_of = factor_of * one(*cut)
    return factor_of


def normal_values(rng, dims, width, reach, cuts=(), kind=jnp.bfloat16):
    values = jax.random.normal(rng, dims, jnp.float32) * width
    if len(cuts) > 0:
        values = level_of(rng, dims, cuts, -0.22, 0.18) * values
    return jnp.clip(values, min=-reach, max=reach).astype(kind)


def setup_inputs(seed: int = 0) -> dict:
    arg_keys = jax.random.split(jax.random.key(seed), 5)
    memory_rows = draw_memory_rows(jax.random.fold_in(arg_keys[4], 71), 0)
    norm_gain = jnp.clip(1.0 + 0.15 * jax.random.normal(arg_keys[1], (D,), jnp.float32), 0.25, 1.75)
    key_weight = normal_values(arg_keys[2], (D, D), D ** -0.5, 0.09375, ((1, 2),))
    owner_table = draw_owner_table(jax.random.fold_in(arg_keys[4], 71), 0)
    return dict(memory_rows=memory_rows, norm_gain=norm_gain, key_weight=key_weight, owner_table=owner_table)


EPS = 1e-05

def reference(memory_rows, norm_gain, key_weight, owner_table):
    values = memory_rows.astype(jnp.float32)
    row_sum = lax.optimization_barrier(jnp.sum(values, axis=1, keepdims=True))
    row_sq = lax.optimization_barrier(jnp.sum(values * values, axis=1, keepdims=True))
    row_mean = row_sum / D
    row_var = row_sq / D - row_mean * row_mean
    normed = ((values - row_mean) * lax.rsqrt(row_var + EPS) * norm_gain[None, :]).astype(jnp.bfloat16)
    keys = jnp.dot(normed, key_weight, preferred_element_type=jnp.float32).astype(jnp.bfloat16)
    blocks = keys.reshape(NB, BLK_ROWS, D)
    placed = jnp.zeros_like(blocks).at[owner_table.astype(jnp.int32)].set(blocks)
    return placed.reshape(ROWS, D)
```

```python
import functools

import jax
import jax.numpy as jnp
from jax import lax
from jax.experimental import pallas as pl
from jax.experimental.pallas import tpu as pltpu
from jax.sharding import PartitionSpec as P

BLK_ROWS = 8
EPS = 1e-05
CHUNKS = 16
LEAD = 4
TAIL = 2
STATS_AT = 4
HALF_AT = 9
SLICE = 256
LANES = 128
LOADS = 8
MIB = 1024 * 1024
MESH = pl.DeviceIdType.MESH


def flipped(me, mask, groups):
    out = me
    bit = 1
    while bit < groups:
        out = out + ((mask // bit) % 2) * bit * (1 - 2 * ((me // bit) % 2))
        bit *= 2
    return out


def mask_at(me, step, groups):
    quarter = groups // 4
    inner = ((me // quarter + 1) // 2) % 2
    turn = step // quarter
    first = (3 - turn) // 3
    second = (turn % 2) * (1 - turn // 2)
    third = (turn // 2) * (1 - turn % 2)
    far = first * (1 + inner) + 3 * second + third * (2 - inner)
    return far * quarter + quarter - 1 - step % quarter


def peer_mask(me, step, groups, early):
    regular = groups - early
    split = groups // 2 - early
    is_early = step // regular
    after = (1 + step // split) // 2
    late = step - regular + split
    return mask_at(me, is_early * late + (1 - is_early) * (step + early * after), groups)


def ranked(offset, value, capacity):
    groups, blocks = offset.shape
    lane = lax.broadcasted_iota(jnp.int32, (groups, blocks), 1)
    chosen = (offset >= 0) & (offset < blocks)
    counted = chosen.astype(jnp.int32)
    shift = 1
    while shift < blocks:
        counted = counted + jnp.where(lane >= shift, pltpu.roll(counted, shift, 1), 0)
        shift *= 2
    result = jnp.zeros((groups, blocks), jnp.int32)
    for r in range(capacity):
        at_rank = jnp.where(chosen & (counted == r + 1), value, 0).astype(jnp.float32)
        found = jnp.sum(at_rank, axis=1, keepdims=True).astype(jnp.int32)
        result = jnp.where(lane == r, found, result)
    return result


def place_kernel(groups, slot_ref, in_ref, out_ref, sem):
    me = lax.axis_index("grp")
    blocks = in_ref.shape[0]
    capacity = blocks // groups

    def move(mask, carry):
        for r in range(capacity):
            slot = slot_ref[me ^ mask, r]
            pltpu.make_async_copy(in_ref.at[mask * capacity + r], out_ref.at[slot], sem).start()
        return carry

    lax.fori_loop(0, groups, move, 0)
    pltpu.make_async_copy(in_ref, out_ref, sem).wait()


def main_kernel(
    groups, parts, table_ref, rows_ref, gain_ref, weight_ref, out_ref, slot_ref,
    table, listed, index, raw, away, mine, others, weight, keys, normed, ready, gains, total,
    columns_stat, own_stat, peer_stat, means, scales,
    table_sem, index_sem, raw_sem, early_send, early_recv, weight_sem, gain_sem, gather_send, gather_recv,
    last_send, last_recv, stat_send, stat_recv, key_send, key_recv,
):
    me = lax.axis_index("grp")
    part = lax.axis_index("tp")
    blocks, _, depth = rows_ref.shape
    row_count = blocks * BLK_ROWS
    width = depth * parts
    chunk = row_count // CHUNKS
    chunk_blocks = blocks // CHUNKS
    capacity = blocks // groups
    per_chunk = groups // CHUNKS
    piece = row_count // groups
    regular = groups - per_chunk
    last = CHUNKS - 1
    body = CHUNKS - TAIL
    tail = TAIL * chunk
    tail_blocks = TAIL * chunk_blocks
    slice_width = min(SLICE, depth)
    slices = depth // slice_width
    sub = 2 * BLK_ROWS

    table_copy = pltpu.make_async_copy(table_ref, table, table_sem)
    table_copy.start()
    loads = min(LOADS, blocks)
    for i in range(loads):
        at = pl.ds(i * (blocks // loads), blocks // loads)
        pltpu.make_async_copy(rows_ref.at[at], raw.at[at], raw_sem).start()
    gain_copy = pltpu.make_async_copy(gain_ref, gains, gain_sem)
    gain_copy.start()

    barrier = pltpu.get_barrier_semaphore()

    def greet(i, carry):
        mask = groups - i
        pl.semaphore_signal(
            barrier, inc=1, device_id={"grp": flipped(me, mask, groups)}, device_id_type=MESH
        )
        return carry

    lax.fori_loop(1, groups, greet, 0)
    for j in range(1, parts):
        pl.semaphore_signal(
            barrier, inc=1, device_id={"tp": (part + j) % parts}, device_id_type=MESH
        )

    def weight_copy(j):
        origin = (part + j) % parts
        return pltpu.make_async_copy(
            weight_ref.at[pl.ds(pl.multiple_of(origin * depth, depth), depth)],
            weight.at[pl.ds(j * depth, depth)],
            weight_sem.at[j],
        )

    def gain_at(j, first, count):
        origin = (part + j) % parts
        return gains[:, pl.ds(pl.multiple_of(origin * depth + first, LANES), count)]

    def gather_copy(c, j):
        at = pl.ds(c * chunk_blocks, chunk_blocks)
        return pltpu.make_async_remote_copy(
            src_ref=mine.at[at],
            dst_ref=others.at[j - 1, at],
            send_sem=gather_send.at[j - 1, c],
            recv_sem=gather_recv.at[j - 1, c],
            device_id={"tp": (part + parts - j) % parts},
            device_id_type=MESH,
        )

    def last_copy(j, s):
        at = pl.ds(body * chunk_blocks, tail_blocks)
        cols = pl.ds(pl.multiple_of(s * slice_width, slice_width), slice_width)
        return pltpu.make_async_remote_copy(
            src_ref=mine.at[at, :, cols],
            dst_ref=others.at[j - 1, at, :, cols],
            send_sem=last_send.at[j - 1, s],
            recv_sem=last_recv.at[j - 1, s],
            device_id={"tp": (part + parts - j) % parts},
            device_id_type=MESH,
        )

    def stat_copy(j):
        return pltpu.make_async_remote_copy(
            src_ref=own_stat,
            dst_ref=peer_stat.at[j - 1],
            send_sem=stat_send.at[j - 1],
            recv_sem=stat_recv.at[j - 1],
            device_id={"tp": (part + parts - j) % parts},
            device_id_type=MESH,
        )

    def key_copy(step):
        mask = peer_mask(me, step, groups, per_chunk)
        return pltpu.make_async_remote_copy(
            src_ref=keys.at[pl.ds(step * piece, piece)],
            dst_ref=out_ref.at[pl.ds(mask * piece, piece)],
            send_sem=key_send.at[step],
            recv_sem=key_recv.at[mask],
            device_id={"grp": flipped(me, mask, groups)},
            device_id_type=MESH,
        )

    def early_copy(i):
        mask = peer_mask(me, regular + i, groups, per_chunk)
        return pltpu.make_async_remote_copy(
            src_ref=away.at[pl.ds(i * capacity, capacity)],
            dst_ref=mine.at[pl.ds((regular + i) * capacity, capacity)],
            send_sem=early_send.at[i],
            recv_sem=early_recv.at[i],
            device_id={"grp": flipped(me, mask, groups)},
            device_id_type=MESH,
        )

    def arrange(c):
        def take(i, carry):
            step = i // capacity
            at = index[step, i - step * capacity]
            block = raw[jnp.minimum(jnp.maximum(at, 0), blocks - 1)]
            if c == last:
                away[i - c * chunk_blocks] = block
            else:
                mine[i] = block
            return carry

        lax.fori_loop(c * chunk_blocks, (c + 1) * chunk_blocks, take, 0, unroll=2)

    row = lax.broadcasted_iota(jnp.int32, (groups, blocks), 0)
    lane = lax.broadcasted_iota(jnp.int32, (groups, blocks), 1)
    peer = jnp.zeros((groups, blocks), jnp.int32)
    for step in range(groups):
        mask = peer_mask(me, step, groups, per_chunk)
        peer = jnp.where(row == step, flipped(me, mask, groups), peer)
    table_copy.wait()
    own = jnp.broadcast_to(table[pl.ds(me, 1), :], (groups, blocks))
    listed[...] = ranked(own - peer * blocks, lane, capacity)
    index_copy = pltpu.make_async_copy(listed, index, index_sem)
    index_copy.start()
    index_copy.wait()
    pltpu.make_async_copy(rows_ref, raw, raw_sem).wait()
    for j in range(parts):
        weight_copy(j).start()

    arrange(0)
    arrange(last)
    pl.semaphore_wait(barrier, groups - 1 + parts - 1)
    for j in range(1, parts):
        gather_copy(0, j).start()
    for i in range(per_chunk):
        early_copy(i).start()
    for c in range(1, last):
        arrange(c)
        if c < LEAD:
            for j in range(1, parts):
                gather_copy(c, j).start()

    offset = table[...] - me * blocks
    slot_ref[...] = ranked(offset, offset, capacity)
    columns_stat[...] = jnp.zeros_like(columns_stat)
    gain_copy.wait()
    for j in range(parts):
        weight_copy(j).wait()

    def stored(c, i, j, first, count):
        at = pl.ds(c * chunk_blocks + i * 2, 2)
        cols = pl.ds(first, count)
        held = mine[at, :, cols] if j == 0 else others[j - 1, at, :, cols]
        return held.astype(jnp.float32).reshape(sub, count)

    def rows_at(i):
        return pl.ds(pl.multiple_of(i * sub, sub), sub)

    def own_sums():
        def sums(i, carry):
            x = stored(body, i, 0, 0, depth)
            row_sum = jnp.sum(x, axis=1, keepdims=True)
            row_sq = jnp.sum(x * x, axis=1, keepdims=True)
            where = lax.broadcasted_iota(jnp.int32, (sub, LANES), 1)
            columns_stat[rows_at(i), :] = jnp.where(
                where == 0, row_sum, jnp.where(where == 1, row_sq, 0.0)
            )
            return carry

        lax.fori_loop(0, tail // sub, sums, 0)
        own_stat[...] = jnp.transpose(columns_stat[...])[:BLK_ROWS]

    def all_sums():
        sums = own_stat[...]
        for j in range(1, parts):
            sums = sums + peer_stat[j - 1]
        columns_stat[:BLK_ROWS, :] = sums
        columns = jnp.transpose(columns_stat[...])[:tail]
        mean = columns[:, 0:1] / width
        means[...] = jnp.broadcast_to(mean, means.shape)
        scale = lax.rsqrt(columns[:, 1:2] / width - mean * mean + EPS)
        scales[...] = jnp.broadcast_to(scale, scales.shape)

    def last_norm(j, first, count):
        def norm_rows(i, carry):
            for k in range(count // LANES):
                at = pl.multiple_of(first + k * LANES, LANES)
                x = stored(body, i, j, at, LANES)
                ready[rows_at(i), pl.ds(pl.multiple_of(j * depth + at, LANES), LANES)] = (
                    (x - means[rows_at(i), :]) * scales[rows_at(i), :] * gain_at(j, at, LANES)
                ).astype(jnp.bfloat16)
            return carry

        lax.fori_loop(0, tail // sub, norm_rows, 0, unroll=count <= SLICE)

    def last_product(j, first, count):
        at = pl.ds(pl.multiple_of(j * depth + first, LANES), count)
        return jnp.dot(ready[:, at], weight[at, :], preferred_element_type=jnp.float32)

    def one_chunk(c, carry):
        base = pl.multiple_of(c * chunk, chunk)

        @pl.when(c == STATS_AT)
        def _():
            for i in range(per_chunk):
                early_copy(i).wait_recv()
            own_sums()
            for j in range(1, parts):
                stat_copy(j).start()

        @pl.when(c == HALF_AT)
        def _():
            for j in range(1, parts):
                stat_copy(j).wait_recv()
            all_sums()
            last_norm(0, 0, depth)
            total[...] = last_product(0, 0, depth)

        for j in range(1, parts):
            gather_copy(c, j).wait_recv()

        @pl.when(c + LEAD < body)
        def _():
            for j in range(1, parts):
                gather_copy(c + LEAD, j).start()

        @pl.when(c + LEAD == body)
        def _():
            def send(s, carry):
                for j in range(1, parts):
                    last_copy(j, s).start()
                return carry

            lax.fori_loop(0, slices, send, 0)

        def norm_rows(i, carry):
            row_sum = 0.0
            row_sq = 0.0
            for j in range(parts):
                x = stored(c, i, j, 0, depth)
                row_sum = row_sum + jnp.sum(x, axis=1, keepdims=True)
                row_sq = row_sq + jnp.sum(x * x, axis=1, keepdims=True)
            mean = row_sum / width
            scale = lax.rsqrt(row_sq / width - mean * mean + EPS)
            for j in range(parts):
                normed[rows_at(i), pl.ds(j * depth, depth)] = (
                    (stored(c, i, j, 0, depth) - mean) * scale * gain_at(j, 0, depth)
                ).astype(jnp.bfloat16)
            return carry

        lax.fori_loop(0, chunk // sub, norm_rows, 0)
        keys[pl.ds(base, chunk), :] = jnp.dot(
            normed[...], weight[...], preferred_element_type=jnp.float32
        ).astype(jnp.bfloat16)

        for i in range(per_chunk):
            key_copy(c * per_chunk + i).start()

        return carry

    lax.fori_loop(0, body, one_chunk, 0)

    def last_slice(s, j):
        first = s * slice_width
        last_copy(j, s).wait_recv()
        last_norm(j, first, slice_width)
        return last_product(j, first, slice_width)

    def add_slice(s, carry):
        for j in range(1, parts):
            total[...] += last_slice(s, j)
        return carry

    lax.fori_loop(0, slices - 1, add_slice, 0)
    for j in range(1, parts - 1):
        total[...] += last_slice(slices - 1, j)
    done = (total[...] + last_slice(slices - 1, parts - 1)).astype(jnp.bfloat16)
    for step in range(body * per_chunk, groups):
        rows = done[step * piece - body * chunk :][:piece]
        if step < regular - 1:
            keys[pl.ds(step * piece, piece), :] = rows
            key_copy(step).start()
        else:
            mask = peer_mask(me, step, groups, per_chunk)
            out_ref[pl.ds(pl.multiple_of(mask * piece, piece), piece), :] = rows

    for i in range(per_chunk):
        early_copy(i).wait_send()
    for j in range(1, parts):
        stat_copy(j).wait_send()

    def sent(c, carry):
        for j in range(1, parts):
            gather_copy(c, j).wait_send()
        return carry

    lax.fori_loop(0, body, sent, 0)

    def last_sent(s, carry):
        for j in range(1, parts):
            last_copy(j, s).wait_send()
        return carry

    lax.fori_loop(0, slices, last_sent, 0)

    def finish(step, carry):
        key_copy(step).wait()
        return carry

    lax.fori_loop(0, regular - 1, finish, 0)


def on_device(groups, parts, memory_rows, norm_gain, key_weight, owner_table):
    row_count, depth = memory_rows.shape
    columns = key_weight.shape[1]
    blocks = row_count // BLK_ROWS
    chunk = row_count // CHUNKS
    per_chunk = groups // CHUNKS
    slices = depth // min(SLICE, depth)
    any_space = pl.BlockSpec(memory_space=pl.ANY)
    in_hbm = pl.BlockSpec(memory_space=pltpu.HBM)
    in_vmem = pl.BlockSpec(memory_space=pltpu.VMEM)
    in_smem = pl.BlockSpec(memory_space=pltpu.SMEM)

    def kept(x):
        return pltpu.with_memory_space_constraint(x, pltpu.HBM)

    dma = pltpu.SemaphoreType.DMA
    incoming, slots = pl.pallas_call(
        functools.partial(main_kernel, groups, parts),
        out_shape=[
            jax.ShapeDtypeStruct((row_count, columns), jnp.bfloat16),
            jax.ShapeDtypeStruct((groups, blocks), jnp.int32),
        ],
        in_specs=[in_hbm, in_hbm, in_hbm, in_hbm],
        out_specs=[in_vmem, in_vmem],
        scratch_shapes=[
            pltpu.VMEM((groups, blocks), jnp.int32),
            pltpu.VMEM((groups, blocks), jnp.int32),
            pltpu.SMEM((groups, blocks), jnp.int32),
            pltpu.VMEM((blocks, BLK_ROWS, depth), jnp.bfloat16),
            pltpu.VMEM((blocks // CHUNKS, BLK_ROWS, depth), jnp.bfloat16),
            pltpu.VMEM((blocks, BLK_ROWS, depth), jnp.bfloat16),
            pltpu.VMEM((parts - 1, blocks, BLK_ROWS, depth), jnp.bfloat16),
            pltpu.VMEM((depth * parts, columns), jnp.bfloat16),
            pltpu.VMEM((row_count, columns), jnp.bfloat16),
            pltpu.VMEM((chunk, depth * parts), jnp.bfloat16),
            pltpu.VMEM((TAIL * chunk, depth * parts), jnp.bfloat16),
            pltpu.VMEM((1, depth * parts), jnp.float32),
            pltpu.VMEM((TAIL * chunk, columns), jnp.float32),
            pltpu.VMEM((LANES, LANES), jnp.float32),
            pltpu.VMEM((BLK_ROWS, LANES), jnp.float32),
            pltpu.VMEM((parts - 1, BLK_ROWS, LANES), jnp.float32),
            pltpu.VMEM((TAIL * chunk, LANES), jnp.float32),
            pltpu.VMEM((TAIL * chunk, LANES), jnp.float32),
            dma,
            dma,
            dma,
            dma((per_chunk,)),
            dma((per_chunk,)),
            dma((parts,)),
            dma,
            dma((parts - 1, CHUNKS)),
            dma((parts - 1, CHUNKS)),
            dma((parts - 1, slices)),
            dma((parts - 1, slices)),
            dma((parts - 1,)),
            dma((parts - 1,)),
            dma((groups,)),
            dma((groups,)),
        ],
        compiler_params=pltpu.CompilerParams(
            collective_id=0, has_side_effects=True, vmem_limit_bytes=48 * MIB
        ),
        name="exchange",
    )(
        kept(owner_table.reshape(groups, blocks)),
        kept(memory_rows.reshape(blocks, BLK_ROWS, depth)),
        kept(norm_gain[None, :]),
        kept(key_weight),
    )

    placed = pl.pallas_call(
        functools.partial(place_kernel, groups),
        out_shape=jax.ShapeDtypeStruct((blocks, BLK_ROWS, columns), jnp.bfloat16),
        in_specs=[in_smem, in_vmem],
        out_specs=any_space,
        scratch_shapes=[pltpu.SemaphoreType.DMA],
        compiler_params=pltpu.CompilerParams(vmem_limit_bytes=16 * MIB),
        name="place",
    )(slots, incoming.reshape(blocks, BLK_ROWS, columns))
    return placed.reshape(row_count, columns)


def solution(mesh):
    in_specs = (P("grp", "tp"), P(), P(None, "tp"), P())
    out_specs = P("grp", "tp")
    return jax.shard_map(
        functools.partial(on_device, mesh.shape["grp"], mesh.shape["tp"]),
        mesh=mesh, in_specs=in_specs, out_specs=out_specs, check_vma=False,
    )
```

```python
import functools

import jax
import jax.numpy as jnp
from jax import lax
from jax.experimental import pallas as pl
from jax.experimental.pallas import tpu as pltpu
from jax.sharding import PartitionSpec as P

BLK_ROWS = 8
EPS = 1e-05
CHUNKS = 16
LEAD = 4
SIDE = 4
TAIL = 2
STATS_AT = 4
HALF_AT = 9
SLICE = 256
LANES = 128
LOADS = 8
MIB = 1024 * 1024
MESH = pl.DeviceIdType.MESH


def flipped(me, mask, groups):
    out = me
    bit = 1
    while bit < groups:
        out = out + ((mask // bit) % 2) * bit * (1 - 2 * ((me // bit) % 2))
        bit *= 2
    return out


def peer_mask(me, step, groups, early):
    quarter = groups // 4
    half = quarter // 2
    one, two, three = ((far + 1) * quarter - 1 for far in (1, 2, 3))
    outer = ((one, quarter), (three, quarter - early), (two, quarter), (quarter - 1, quarter))
    inner = (
        (two, quarter), (quarter - 1, half), (three, quarter - early), (one, quarter), (half - 1, half)
    )

    def mask_in(runs):
        out = 0
        begin = 0
        for first, length in (*runs, (3 * quarter + early - 1, early)):
            out = jnp.where(step >= begin, first + begin - step, out)
            begin += length
        return out

    middle = ((me // quarter + 1) // 2) % 2
    return jnp.where(middle == 1, mask_in(inner), mask_in(outer))


def ranked(offset, value, capacity):
    groups, blocks = offset.shape
    lane = lax.broadcasted_iota(jnp.int32, (groups, blocks), 1)
    chosen = (offset >= 0) & (offset < blocks)
    counted = chosen.astype(jnp.int32)
    shift = 1
    while shift < blocks:
        counted = counted + jnp.where(lane >= shift, pltpu.roll(counted, shift, 1), 0)
        shift *= 2
    result = jnp.zeros((groups, blocks), jnp.int32)
    for r in range(capacity):
        at_rank = jnp.where(chosen & (counted == r + 1), value, 0).astype(jnp.float32)
        found = jnp.sum(at_rank, axis=1, keepdims=True).astype(jnp.int32)
        result = jnp.where(lane == r, found, result)
    return result


def place_kernel(groups, slot_ref, in_ref, out_ref, sem):
    me = lax.axis_index("grp")
    blocks = in_ref.shape[0]
    capacity = blocks // groups

    def move(mask, carry):
        for r in range(capacity):
            slot = slot_ref[me ^ mask, r]
            pltpu.make_async_copy(in_ref.at[mask * capacity + r], out_ref.at[slot], sem).start()
        return carry

    lax.fori_loop(0, groups, move, 0)
    pltpu.make_async_copy(in_ref, out_ref, sem).wait()


def main_kernel(
    groups, parts, table_ref, rows_ref, gain_ref, weight_ref, out_ref, slot_ref,
    table, listed, index, raw, away, mine, others, weight, keys, normed, ready, gains, total,
    columns_stat, own_stat, peer_stat, means, scales,
    table_sem, index_sem, raw_sem, early_send, early_recv, weight_sem, gain_sem, gather_send, gather_recv,
    last_send, last_recv, stat_send, stat_recv, key_send, key_recv, met,
):
    me = lax.axis_index("grp")
    part = lax.axis_index("tp")
    blocks, _, depth = rows_ref.shape
    row_count = blocks * BLK_ROWS
    width = depth * parts
    chunk = row_count // CHUNKS
    chunk_blocks = blocks // CHUNKS
    capacity = blocks // groups
    per_chunk = groups // CHUNKS
    piece = row_count // groups
    regular = groups - per_chunk
    last = CHUNKS - 1
    body = CHUNKS - TAIL
    tail = TAIL * chunk
    tail_blocks = TAIL * chunk_blocks
    slice_width = min(SLICE, depth)
    slices = depth // slice_width
    sub = 2 * BLK_ROWS

    table_copy = pltpu.make_async_copy(table_ref, table, table_sem)
    table_copy.start()
    line = me // SIDE
    lines = groups // SIDE
    loads = min(LOADS, blocks)
    for i in range(loads):
        at = pl.ds(i * (blocks // loads), blocks // loads)
        pltpu.make_async_copy(rows_ref.at[at], raw.at[at], raw_sem).start()
    gain_copy = pltpu.make_async_copy(gain_ref, gains, gain_sem)
    gain_copy.start()

    barrier = pltpu.get_barrier_semaphore()

    def greet(sem, device):
        pl.semaphore_signal(sem, inc=1, device_id=device, device_id_type=MESH)

    for j in range(1, parts):
        greet(barrier, {"tp": (part + j) % parts})
    for bit in range(2):
        greet(barrier, {"grp": flipped(me, 1 << bit, SIDE)})

    @pl.when(line > 0)
    def _():
        greet(barrier, {"grp": me - SIDE})

    @pl.when(line < lines - 1)
    def _():
        greet(barrier, {"grp": me + SIDE})

    def weight_copy(j):
        origin = (part + j) % parts
        return pltpu.make_async_copy(
            weight_ref.at[pl.ds(pl.multiple_of(origin * depth, depth), depth)],
            weight.at[pl.ds(j * depth, depth)],
            weight_sem.at[j],
        )

    def gain_at(j, first, count):
        origin = (part + j) % parts
        return gains[:, pl.ds(pl.multiple_of(origin * depth + first, LANES), count)]

    def gather_copy(c, j):
        at = pl.ds(c * chunk_blocks, chunk_blocks)
        return pltpu.make_async_remote_copy(
            src_ref=mine.at[at],
            dst_ref=others.at[j - 1, at],
            send_sem=gather_send.at[j - 1, c],
            recv_sem=gather_recv.at[j - 1, c],
            device_id={"tp": (part + parts - j) % parts},
            device_id_type=MESH,
        )

    def last_copy(j, s):
        at = pl.ds(body * chunk_blocks, tail_blocks)
        cols = pl.ds(pl.multiple_of(s * slice_width, slice_width), slice_width)
        return pltpu.make_async_remote_copy(
            src_ref=mine.at[at, :, cols],
            dst_ref=others.at[j - 1, at, :, cols],
            send_sem=last_send.at[j - 1, s],
            recv_sem=last_recv.at[j - 1, s],
            device_id={"tp": (part + parts - j) % parts},
            device_id_type=MESH,
        )

    def stat_copy(j):
        return pltpu.make_async_remote_copy(
            src_ref=own_stat,
            dst_ref=peer_stat.at[j - 1],
            send_sem=stat_send.at[j - 1],
            recv_sem=stat_recv.at[j - 1],
            device_id={"tp": (part + parts - j) % parts},
            device_id_type=MESH,
        )

    def key_copy(step):
        mask = peer_mask(me, step, groups, per_chunk)
        return pltpu.make_async_remote_copy(
            src_ref=keys.at[pl.ds(step * piece, piece)],
            dst_ref=out_ref.at[pl.ds(mask * piece, piece)],
            send_sem=key_send.at[step],
            recv_sem=key_recv.at[mask],
            device_id={"grp": flipped(me, mask, groups)},
            device_id_type=MESH,
        )

    def early_copy(i):
        mask = peer_mask(me, regular + i, groups, per_chunk)
        return pltpu.make_async_remote_copy(
            src_ref=away.at[pl.ds(i * capacity, capacity)],
            dst_ref=mine.at[pl.ds((regular + i) * capacity, capacity)],
            send_sem=early_send.at[i],
            recv_sem=early_recv.at[i],
            device_id={"grp": flipped(me, mask, groups)},
            device_id_type=MESH,
        )

    def arrange(c):
        def take(i, carry):
            step = i // capacity
            at = index[step, i - step * capacity]
            block = raw[jnp.minimum(jnp.maximum(at, 0), blocks - 1)]
            if c == last:
                away[i - c * chunk_blocks] = block
            else:
                mine[i] = block
            return carry

        lax.fori_loop(c * chunk_blocks, (c + 1) * chunk_blocks, take, 0, unroll=2)

    row = lax.broadcasted_iota(jnp.int32, (groups, blocks), 0)
    lane = lax.broadcasted_iota(jnp.int32, (groups, blocks), 1)
    peer = jnp.zeros((groups, blocks), jnp.int32)
    for step in range(groups):
        mask = peer_mask(me, step, groups, per_chunk)
        peer = jnp.where(row == step, flipped(me, mask, groups), peer)
    table_copy.wait()
    own = jnp.broadcast_to(table[pl.ds(me, 1), :], (groups, blocks))
    listed[...] = ranked(own - peer * blocks, lane, capacity)
    index_copy = pltpu.make_async_copy(listed, index, index_sem)
    index_copy.start()
    index_copy.wait()
    pltpu.make_async_copy(rows_ref, raw, raw_sem).wait()
    for j in range(parts):
        weight_copy(j).start()

    arrange(0)
    arrange(last)
    inner = (line > 0) & (line < lines - 1)
    neighbours = 1 + inner.astype(jnp.int32)
    pl.semaphore_wait(barrier, parts - 1 + 2 + neighbours)

    def gather(c):
        for j in range(1, parts):
            gather_copy(c, j).start()

    def send_early():
        for i in range(per_chunk):
            early_copy(i).start()

    gather(0)
    near = lines == 4 and per_chunk == 1
    if near:

        @pl.when(inner)
        def _():
            send_early()

    arrange(1)
    gather(1)

    def from_below():
        @pl.when(line > 1)
        def _():
            pl.semaphore_wait(met.at[0], 1)

        @pl.when((line > 0) & (line < lines - 1))
        def _():
            greet(met.at[0], {"grp": me + SIDE})

    def from_above():
        @pl.when(line < lines - 2)
        def _():
            pl.semaphore_wait(met.at[1], 1)

        @pl.when((line > 0) & (line < lines - 1))
        def _():
            greet(met.at[1], {"grp": me - SIDE})

    @pl.when(line < lines // 2)
    def _():
        from_below()
        from_above()

    @pl.when(line >= lines // 2)
    def _():
        from_above()
        from_below()

    if near:

        @pl.when(jnp.logical_not(inner))
        def _():
            send_early()

    for bit in range(2):
        greet(met.at[2 + bit], {"grp": flipped(me, 1 << bit, SIDE)})
        pl.semaphore_wait(met.at[2 + bit], 1)
    if not near:
        send_early()
    for c in range(2, last):
        arrange(c)
        if c < LEAD:
            gather(c)

    offset = table[...] - me * blocks
    slot_ref[...] = ranked(offset, offset, capacity)
    columns_stat[...] = jnp.zeros_like(columns_stat)
    gain_copy.wait()
    for j in range(parts):
        weight_copy(j).wait()

    def stored(c, i, j, first, count):
        at = pl.ds(c * chunk_blocks + i * 2, 2)
        cols = pl.ds(first, count)
        held = mine[at, :, cols] if j == 0 else others[j - 1, at, :, cols]
        return held.astype(jnp.float32).reshape(sub, count)

    def rows_at(i):
        return pl.ds(pl.multiple_of(i * sub, sub), sub)

    def own_sums():
        def sums(i, carry):
            x = stored(body, i, 0, 0, depth)
            row_sum = jnp.sum(x, axis=1, keepdims=True)
            row_sq = jnp.sum(x * x, axis=1, keepdims=True)
            where = lax.broadcasted_iota(jnp.int32, (sub, LANES), 1)
            columns_stat[rows_at(i), :] = jnp.where(
                where == 0, row_sum, jnp.where(where == 1, row_sq, 0.0)
            )
            return carry

        lax.fori_loop(0, tail // sub, sums, 0)
        own_stat[...] = jnp.transpose(columns_stat[...])[:BLK_ROWS]

    def all_sums():
        sums = own_stat[...]
        for j in range(1, parts):
            sums = sums + peer_stat[j - 1]
        columns_stat[:BLK_ROWS, :] = sums
        columns = jnp.transpose(columns_stat[...])[:tail]
        mean = columns[:, 0:1] / width
        means[...] = jnp.broadcast_to(mean, means.shape)
        scale = lax.rsqrt(columns[:, 1:2] / width - mean * mean + EPS)
        scales[...] = jnp.broadcast_to(scale, scales.shape)

    def last_norm(j, first, count):
        def norm_rows(i, carry):
            for k in range(count // LANES):
                at = pl.multiple_of(first + k * LANES, LANES)
                x = stored(body, i, j, at, LANES)
                ready[rows_at(i), pl.ds(pl.multiple_of(j * depth + at, LANES), LANES)] = (
                    (x - means[rows_at(i), :]) * scales[rows_at(i), :] * gain_at(j, at, LANES)
                ).astype(jnp.bfloat16)
            return carry

        lax.fori_loop(0, tail // sub, norm_rows, 0, unroll=count <= SLICE)

    def last_product(j, first, count):
        at = pl.ds(pl.multiple_of(j * depth + first, LANES), count)
        return jnp.dot(ready[:, at], weight[at, :], preferred_element_type=jnp.float32)

    def one_chunk(c, carry):
        base = pl.multiple_of(c * chunk, chunk)

        @pl.when(c == STATS_AT)
        def _():
            for i in range(per_chunk):
                early_copy(i).wait_recv()
            own_sums()
            for j in range(1, parts):
                stat_copy(j).start()

        @pl.when(c == HALF_AT)
        def _():
            for j in range(1, parts):
                stat_copy(j).wait_recv()
            all_sums()
            last_norm(0, 0, depth)
            total[...] = last_product(0, 0, depth)

        for j in range(1, parts):
            gather_copy(c, j).wait_recv()

        @pl.when(c + LEAD < body)
        def _():
            for j in range(1, parts):
                gather_copy(c + LEAD, j).start()

        @pl.when(c + LEAD == body)
        def _():
            def send(s, carry):
                for j in range(1, parts):
                    last_copy(j, s).start()
                return carry

            lax.fori_loop(0, slices, send, 0)

        def norm_rows(i, carry):
            row_sum = 0.0
            row_sq = 0.0
            for j in range(parts):
                x = stored(c, i, j, 0, depth)
                row_sum = row_sum + jnp.sum(x, axis=1, keepdims=True)
                row_sq = row_sq + jnp.sum(x * x, axis=1, keepdims=True)
            mean = row_sum / width
            scale = lax.rsqrt(row_sq / width - mean * mean + EPS)
            for j in range(parts):
                normed[rows_at(i), pl.ds(j * depth, depth)] = (
                    (stored(c, i, j, 0, depth) - mean) * scale * gain_at(j, 0, depth)
                ).astype(jnp.bfloat16)
            return carry

        lax.fori_loop(0, chunk // sub, norm_rows, 0)
        keys[pl.ds(base, chunk), :] = jnp.dot(
            normed[...], weight[...], preferred_element_type=jnp.float32
        ).astype(jnp.bfloat16)

        for i in range(per_chunk):
            key_copy(c * per_chunk + i).start()

        return carry

    lax.fori_loop(0, body, one_chunk, 0)

    def last_slice(s, j):
        first = s * slice_width
        last_copy(j, s).wait_recv()
        last_norm(j, first, slice_width)
        return last_product(j, first, slice_width)

    def add_slice(s, carry):
        for j in range(1, parts):
            total[...] += last_slice(s, j)
        return carry

    lax.fori_loop(0, slices - 1, add_slice, 0)
    for j in range(1, parts - 1):
        total[...] += last_slice(slices - 1, j)
    done = (total[...] + last_slice(slices - 1, parts - 1)).astype(jnp.bfloat16)
    for step in range(body * per_chunk, groups):
        rows = done[step * piece - body * chunk :][:piece]
        if step < regular - 1:
            keys[pl.ds(step * piece, piece), :] = rows
            key_copy(step).start()
        else:
            mask = peer_mask(me, step, groups, per_chunk)
            out_ref[pl.ds(pl.multiple_of(mask * piece, piece), piece), :] = rows

    for i in range(per_chunk):
        early_copy(i).wait_send()
    for j in range(1, parts):
        stat_copy(j).wait_send()

    def sent(c, carry):
        for j in range(1, parts):
            gather_copy(c, j).wait_send()
        return carry

    lax.fori_loop(0, body, sent, 0)

    def last_sent(s, carry):
        for j in range(1, parts):
            last_copy(j, s).wait_send()
        return carry

    lax.fori_loop(0, slices, last_sent, 0)

    def finish(step, carry):
        key_copy(step).wait()
        return carry

    lax.fori_loop(0, regular - 1, finish, 0)


def on_device(groups, parts, memory_rows, norm_gain, key_weight, owner_table):
    row_count, depth = memory_rows.shape
    columns = key_weight.shape[1]
    blocks = row_count // BLK_ROWS
    chunk = row_count // CHUNKS
    per_chunk = groups // CHUNKS
    slices = depth // min(SLICE, depth)
    any_space = pl.BlockSpec(memory_space=pl.ANY)
    in_hbm = pl.BlockSpec(memory_space=pltpu.HBM)
    in_vmem = pl.BlockSpec(memory_space=pltpu.VMEM)
    in_smem = pl.BlockSpec(memory_space=pltpu.SMEM)

    def kept(x):
        return pltpu.with_memory_space_constraint(x, pltpu.HBM)

    dma = pltpu.SemaphoreType.DMA
    incoming, slots = pl.pallas_call(
        functools.partial(main_kernel, groups, parts),
        out_shape=[
            jax.ShapeDtypeStruct((row_count, columns), jnp.bfloat16),
            jax.ShapeDtypeStruct((groups, blocks), jnp.int32),
        ],
        in_specs=[in_hbm, in_hbm, in_hbm, in_hbm],
        out_specs=[in_vmem, in_vmem],
        scratch_shapes=[
            pltpu.VMEM((groups, blocks), jnp.int32),
            pltpu.VMEM((groups, blocks), jnp.int32),
            pltpu.SMEM((groups, blocks), jnp.int32),
            pltpu.VMEM((blocks, BLK_ROWS, depth), jnp.bfloat16),
            pltpu.VMEM((blocks // CHUNKS, BLK_ROWS, depth), jnp.bfloat16),
            pltpu.VMEM((blocks, BLK_ROWS, depth), jnp.bfloat16),
            pltpu.VMEM((parts - 1, blocks, BLK_ROWS, depth), jnp.bfloat16),
            pltpu.VMEM((depth * parts, columns), jnp.bfloat16),
            pltpu.VMEM((row_count, columns), jnp.bfloat16),
            pltpu.VMEM((chunk, depth * parts), jnp.bfloat16),
            pltpu.VMEM((TAIL * chunk, depth * parts), jnp.bfloat16),
            pltpu.VMEM((1, depth * parts), jnp.float32),
            pltpu.VMEM((TAIL * chunk, columns), jnp.float32),
            pltpu.VMEM((LANES, LANES), jnp.float32),
            pltpu.VMEM((BLK_ROWS, LANES), jnp.float32),
            pltpu.VMEM((parts - 1, BLK_ROWS, LANES), jnp.float32),
            pltpu.VMEM((TAIL * chunk, LANES), jnp.float32),
            pltpu.VMEM((TAIL * chunk, LANES), jnp.float32),
            dma,
            dma,
            dma,
            dma((per_chunk,)),
            dma((per_chunk,)),
            dma((parts,)),
            dma,
            dma((parts - 1, CHUNKS)),
            dma((parts - 1, CHUNKS)),
            dma((parts - 1, slices)),
            dma((parts - 1, slices)),
            dma((parts - 1,)),
            dma((parts - 1,)),
            dma((groups,)),
            dma((groups,)),
            pltpu.SemaphoreType.REGULAR((4,)),
        ],
        compiler_params=pltpu.CompilerParams(
            collective_id=0, has_side_effects=True, vmem_limit_bytes=48 * MIB
        ),
        name="exchange",
    )(
        kept(owner_table.reshape(groups, blocks)),
        kept(memory_rows.reshape(blocks, BLK_ROWS, depth)),
        kept(norm_gain[None, :]),
        kept(key_weight),
    )

    placed = pl.pallas_call(
        functools.partial(place_kernel, groups),
        out_shape=jax.ShapeDtypeStruct((blocks, BLK_ROWS, columns), jnp.bfloat16),
        in_specs=[in_smem, in_vmem],
        out_specs=any_space,
        scratch_shapes=[pltpu.SemaphoreType.DMA],
        compiler_params=pltpu.CompilerParams(vmem_limit_bytes=16 * MIB),
        name="place",
    )(slots, incoming.reshape(blocks, BLK_ROWS, columns))
    return placed.reshape(row_count, columns)


def solution(mesh):
    in_specs = (P("grp", "tp"), P(), P(None, "tp"), P())
    out_specs = P("grp", "tp")
    return jax.shard_map(
        functools.partial(on_device, mesh.shape["grp"], mesh.shape["tp"]),
        mesh=mesh, in_specs=in_specs, out_specs=out_specs, check_vma=False,
    )
```

```python
import functools

import jax
import jax.numpy as jnp
from jax import lax
from jax.experimental import pallas as pl
from jax.experimental.pallas import tpu as pltpu
from jax.sharding import PartitionSpec as P

BLK_ROWS = 8
EPS = 1e-05
CHUNKS = 16
LEAD = 4
SIDE = 4
TAIL = 2
STATS_AT = 4
HALF_AT = 9
SLICE = 256
LANES = 128
LOADS = 8
MIB = 1024 * 1024
MESH = pl.DeviceIdType.MESH


def flipped(me, mask, groups):
    out = me
    bit = 1
    while bit < groups:
        out = out + ((mask // bit) % 2) * bit * (1 - 2 * ((me // bit) % 2))
        bit *= 2
    return out


def peer_mask(me, step, groups, early):
    quarter = groups // 4
    half = quarter // 2
    one, two, three = ((far + 1) * quarter - 1 for far in (1, 2, 3))
    outer = ((one, quarter), (three, quarter - early), (two, quarter), (quarter - 1, quarter))
    inner = (
        (two, quarter), (quarter - 1, half), (three, quarter - early), (one, quarter), (half - 1, half)
    )

    def mask_in(runs):
        out = 0
        begin = 0
        for first, length in (*runs, (3 * quarter + early - 1, early)):
            out = jnp.where(step >= begin, first + begin - step, out)
            begin += length
        return out

    middle = ((me // quarter + 1) // 2) % 2
    return jnp.where(middle == 1, mask_in(inner), mask_in(outer))


def ranked(offset, value, capacity):
    groups, blocks = offset.shape
    lane = lax.broadcasted_iota(jnp.int32, (groups, blocks), 1)
    chosen = (offset >= 0) & (offset < blocks)
    counted = chosen.astype(jnp.int32)
    shift = 1
    while shift < blocks:
        counted = counted + jnp.where(lane >= shift, pltpu.roll(counted, shift, 1), 0)
        shift *= 2
    result = jnp.zeros((groups, blocks), jnp.int32)
    for r in range(capacity):
        at_rank = jnp.where(chosen & (counted == r + 1), value, 0).astype(jnp.float32)
        found = jnp.sum(at_rank, axis=1, keepdims=True).astype(jnp.int32)
        result = jnp.where(lane == r, found, result)
    return result


def place_kernel(groups, slot_ref, in_ref, out_ref, sem):
    me = lax.axis_index("grp")
    blocks = in_ref.shape[0]
    capacity = blocks // groups
    for mask in range(groups):
        slots = slot_ref[pl.ds(me ^ mask, 1), :]
        for r in range(capacity):
            pltpu.make_async_copy(
                in_ref.at[mask * capacity + r], out_ref.at[slots[0, r]], sem
            ).start()
    pltpu.make_async_copy(in_ref, out_ref, sem).wait()


def main_kernel(
    groups, parts, table_ref, rows_ref, gain_ref, weight_ref, out_ref, slot_ref,
    table, listed, index, raw, away, mine, others, weight, keys, normed, ready, gains, total,
    columns_stat, own_stat, peer_stat, means, scales,
    table_sem, index_sem, raw_sem, early_send, early_recv, weight_sem, gain_sem, gather_send, gather_recv,
    last_send, last_recv, stat_send, stat_recv, key_send, key_recv, met,
):
    me = lax.axis_index("grp")
    part = lax.axis_index("tp")
    blocks, _, depth = rows_ref.shape
    row_count = blocks * BLK_ROWS
    width = depth * parts
    chunk = row_count // CHUNKS
    chunk_blocks = blocks // CHUNKS
    capacity = blocks // groups
    per_chunk = groups // CHUNKS
    piece = row_count // groups
    regular = groups - per_chunk
    last = CHUNKS - 1
    body = CHUNKS - TAIL
    tail = TAIL * chunk
    tail_blocks = TAIL * chunk_blocks
    slice_width = min(SLICE, depth)
    slices = depth // slice_width
    sub = 2 * BLK_ROWS

    table_copy = pltpu.make_async_copy(table_ref, table, table_sem)
    table_copy.start()
    line = me // SIDE
    lines = groups // SIDE
    loads = min(LOADS, blocks)
    for i in range(loads):
        at = pl.ds(i * (blocks // loads), blocks // loads)
        pltpu.make_async_copy(rows_ref.at[at], raw.at[at], raw_sem).start()
    gain_copy = pltpu.make_async_copy(gain_ref, gains, gain_sem)
    gain_copy.start()

    barrier = pltpu.get_barrier_semaphore()

    def greet(sem, device):
        pl.semaphore_signal(sem, inc=1, device_id=device, device_id_type=MESH)

    for j in range(1, parts):
        greet(barrier, {"tp": (part + j) % parts})
    for bit in range(2):
        greet(barrier, {"grp": flipped(me, 1 << bit, SIDE)})

    @pl.when(line > 0)
    def _():
        greet(barrier, {"grp": me - SIDE})

    @pl.when(line < lines - 1)
    def _():
        greet(barrier, {"grp": me + SIDE})

    def weight_copy(j):
        origin = (part + j) % parts
        return pltpu.make_async_copy(
            weight_ref.at[pl.ds(pl.multiple_of(origin * depth, depth), depth)],
            weight.at[pl.ds(j * depth, depth)],
            weight_sem.at[j],
        )

    def gain_at(j, first, count):
        origin = (part + j) % parts
        return gains[:, pl.ds(pl.multiple_of(origin * depth + first, LANES), count)]

    def gather_copy(c, j):
        at = pl.ds(c * chunk_blocks, chunk_blocks)
        return pltpu.make_async_remote_copy(
            src_ref=mine.at[at],
            dst_ref=others.at[j - 1, at],
            send_sem=gather_send.at[j - 1, c],
            recv_sem=gather_recv.at[j - 1, c],
            device_id={"tp": (part + parts - j) % parts},
            device_id_type=MESH,
        )

    def last_copy(j, s):
        at = pl.ds(body * chunk_blocks, tail_blocks)
        cols = pl.ds(pl.multiple_of(s * slice_width, slice_width), slice_width)
        return pltpu.make_async_remote_copy(
            src_ref=mine.at[at, :, cols],
            dst_ref=others.at[j - 1, at, :, cols],
            send_sem=last_send.at[j - 1, s],
            recv_sem=last_recv.at[j - 1, s],
            device_id={"tp": (part + parts - j) % parts},
            device_id_type=MESH,
        )

    def stat_copy(j):
        return pltpu.make_async_remote_copy(
            src_ref=own_stat,
            dst_ref=peer_stat.at[j - 1],
            send_sem=stat_send.at[j - 1],
            recv_sem=stat_recv.at[j - 1],
            device_id={"tp": (part + parts - j) % parts},
            device_id_type=MESH,
        )

    def key_copy(step):
        mask = peer_mask(me, step, groups, per_chunk)
        return pltpu.make_async_remote_copy(
            src_ref=keys.at[pl.ds(step * piece, piece)],
            dst_ref=out_ref.at[pl.ds(mask * piece, piece)],
            send_sem=key_send.at[step],
            recv_sem=key_recv.at[mask],
            device_id={"grp": flipped(me, mask, groups)},
            device_id_type=MESH,
        )

    def key_wait(step, mask):
        return pltpu.make_async_remote_copy(
            src_ref=keys.at[pl.ds(step * piece, piece)],
            dst_ref=out_ref.at[pl.ds(mask * piece, piece)],
            send_sem=key_send.at[step],
            recv_sem=key_recv.at[mask],
            device_id={"grp": flipped(me, 1, SIDE)},
            device_id_type=MESH,
        )

    def early_copy(i):
        mask = peer_mask(me, regular + i, groups, per_chunk)
        return pltpu.make_async_remote_copy(
            src_ref=away.at[pl.ds(i * capacity, capacity)],
            dst_ref=mine.at[pl.ds((regular + i) * capacity, capacity)],
            send_sem=early_send.at[i],
            recv_sem=early_recv.at[i],
            device_id={"grp": flipped(me, mask, groups)},
            device_id_type=MESH,
        )

    def arrange(c):
        def take(i, carry):
            step = i // capacity
            at = index[step, i - step * capacity]
            block = raw[jnp.minimum(jnp.maximum(at, 0), blocks - 1)]
            if c == last:
                away[i - c * chunk_blocks] = block
            else:
                mine[i] = block
            return carry

        lax.fori_loop(c * chunk_blocks, (c + 1) * chunk_blocks, take, 0, unroll=2)

    row = lax.broadcasted_iota(jnp.int32, (groups, blocks), 0)
    lane = lax.broadcasted_iota(jnp.int32, (groups, blocks), 1)
    peer = jnp.zeros((groups, blocks), jnp.int32)
    for step in range(groups):
        mask = peer_mask(me, step, groups, per_chunk)
        peer = jnp.where(row == step, flipped(me, mask, groups), peer)
    table_copy.wait()
    own = jnp.broadcast_to(table[pl.ds(me, 1), :], (groups, blocks))
    listed[...] = ranked(own - peer * blocks, lane, capacity)
    index_copy = pltpu.make_async_copy(listed, index, index_sem)
    index_copy.start()
    pltpu.make_async_copy(rows_ref, raw, raw_sem).wait()
    for j in range(parts):
        weight_copy(j).start()

    for i in range(chunk_blocks):
        at = listed[pl.ds(i // capacity, 1), pl.ds(i % capacity, 1)][0, 0]
        mine[i] = raw[jnp.minimum(jnp.maximum(at, 0), blocks - 1)]
    inner = (line > 0) & (line < lines - 1)
    neighbours = 1 + inner.astype(jnp.int32)
    pl.semaphore_wait(barrier, parts - 1 + 2 + neighbours)

    def gather(c):
        for j in range(1, parts):
            gather_copy(c, j).start()

    def send_early():
        for i in range(per_chunk):
            early_copy(i).start()

    gather(0)
    index_copy.wait()
    arrange(last)
    near = lines == 4 and per_chunk == 1
    if near:

        @pl.when(inner)
        def _():
            send_early()

    arrange(1)
    gather(1)

    def from_below():
        @pl.when(line > 1)
        def _():
            pl.semaphore_wait(met.at[0], 1)

        @pl.when((line > 0) & (line < lines - 1))
        def _():
            greet(met.at[0], {"grp": me + SIDE})

    def from_above():
        @pl.when(line < lines - 2)
        def _():
            pl.semaphore_wait(met.at[1], 1)

        @pl.when((line > 0) & (line < lines - 1))
        def _():
            greet(met.at[1], {"grp": me - SIDE})

    @pl.when(line < lines // 2)
    def _():
        from_below()
        from_above()

    @pl.when(line >= lines // 2)
    def _():
        from_above()
        from_below()

    if near:

        @pl.when(jnp.logical_not(inner))
        def _():
            send_early()

    for bit in range(2):
        greet(met.at[2 + bit], {"grp": flipped(me, 1 << bit, SIDE)})
        pl.semaphore_wait(met.at[2 + bit], 1)
    if not near:
        send_early()
    for c in range(2, last):
        arrange(c)
        if c < LEAD:
            gather(c)

    offset = table[...] - me * blocks
    slot_ref[...] = ranked(offset, offset, capacity)
    columns_stat[...] = jnp.zeros_like(columns_stat)
    gain_copy.wait()
    for j in range(parts):
        weight_copy(j).wait()

    def stored(c, i, j, first, count):
        at = pl.ds(c * chunk_blocks + i * 2, 2)
        cols = pl.ds(first, count)
        held = mine[at, :, cols] if j == 0 else others[j - 1, at, :, cols]
        return held.astype(jnp.float32).reshape(sub, count)

    def rows_at(i):
        return pl.ds(pl.multiple_of(i * sub, sub), sub)

    def own_sums():
        def sums(i, carry):
            x = stored(body, i, 0, 0, depth)
            row_sum = jnp.sum(x, axis=1, keepdims=True)
            row_sq = jnp.sum(x * x, axis=1, keepdims=True)
            where = lax.broadcasted_iota(jnp.int32, (sub, LANES), 1)
            columns_stat[rows_at(i), :] = jnp.where(
                where == 0, row_sum, jnp.where(where == 1, row_sq, 0.0)
            )
            return carry

        lax.fori_loop(0, tail // sub, sums, 0)
        own_stat[...] = jnp.transpose(columns_stat[...])[:BLK_ROWS]

    def all_sums():
        sums = own_stat[...]
        for j in range(1, parts):
            sums = sums + peer_stat[j - 1]
        columns_stat[:BLK_ROWS, :] = sums
        columns = jnp.transpose(columns_stat[...])[:tail]
        mean = columns[:, 0:1] / width
        means[...] = jnp.broadcast_to(mean, means.shape)
        scale = lax.rsqrt(columns[:, 1:2] / width - mean * mean + EPS)
        scales[...] = jnp.broadcast_to(scale, scales.shape)

    def last_norm(j, first, count):
        def norm_rows(i, carry):
            for k in range(count // LANES):
                at = pl.multiple_of(first + k * LANES, LANES)
                x = stored(body, i, j, at, LANES)
                ready[rows_at(i), pl.ds(pl.multiple_of(j * depth + at, LANES), LANES)] = (
                    (x - means[rows_at(i), :]) * scales[rows_at(i), :] * gain_at(j, at, LANES)
                ).astype(jnp.bfloat16)
            return carry

        lax.fori_loop(0, tail // sub, norm_rows, 0, unroll=count <= SLICE)

    def last_product(j, first, count):
        at = pl.ds(pl.multiple_of(j * depth + first, LANES), count)
        return jnp.dot(ready[:, at], weight[at, :], preferred_element_type=jnp.float32)

    def one_chunk(c, carry):
        base = pl.multiple_of(c * chunk, chunk)

        @pl.when(c == STATS_AT)
        def _():
            for i in range(per_chunk):
                early_copy(i).wait_recv()
            own_sums()
            for j in range(1, parts):
                stat_copy(j).start()

        @pl.when(c == HALF_AT)
        def _():
            for j in range(1, parts):
                stat_copy(j).wait_recv()
            all_sums()
            last_norm(0, 0, depth)
            total[...] = last_product(0, 0, depth)

        for j in range(1, parts):
            gather_copy(c, j).wait_recv()

        @pl.when(c + LEAD < body)
        def _():
            for j in range(1, parts):
                gather_copy(c + LEAD, j).start()

        @pl.when(c + LEAD == body)
        def _():
            def send(s, carry):
                for j in range(1, parts):
                    last_copy(j, s).start()
                return carry

            lax.fori_loop(0, slices, send, 0)

        def norm_rows(i, carry):
            row_sum = 0.0
            row_sq = 0.0
            for j in range(parts):
                x = stored(c, i, j, 0, depth)
                row_sum = row_sum + jnp.sum(x, axis=1, keepdims=True)
                row_sq = row_sq + jnp.sum(x * x, axis=1, keepdims=True)
            mean = row_sum / width
            scale = lax.rsqrt(row_sq / width - mean * mean + EPS)
            for j in range(parts):
                normed[rows_at(i), pl.ds(j * depth, depth)] = (
                    (stored(c, i, j, 0, depth) - mean) * scale * gain_at(j, 0, depth)
                ).astype(jnp.bfloat16)
            return carry

        lax.fori_loop(0, chunk // sub, norm_rows, 0)
        keys[pl.ds(base, chunk), :] = jnp.dot(
            normed[...], weight[...], preferred_element_type=jnp.float32
        ).astype(jnp.bfloat16)

        for i in range(per_chunk):
            key_copy(c * per_chunk + i).start()

        return carry

    lax.fori_loop(0, body, one_chunk, 0)

    for i in range(per_chunk):
        early_copy(i).wait_send()
    for j in range(1, parts):
        stat_copy(j).wait_send()

    def sent(c, carry):
        for j in range(1, parts):
            gather_copy(c, j).wait_send()
        return carry

    lax.fori_loop(0, body, sent, 0)

    def last_slice(s, j):
        first = s * slice_width
        last_copy(j, s).wait_recv()
        last_norm(j, first, slice_width)
        return last_product(j, first, slice_width)

    def add_slice(s, carry):
        for j in range(1, parts):
            total[...] += last_slice(s, j)
        return carry

    lax.fori_loop(0, slices - 1, add_slice, 0)
    for j in range(1, parts - 1):
        total[...] += last_slice(slices - 1, j)
    done = (total[...] + last_slice(slices - 1, parts - 1)).astype(jnp.bfloat16)
    for step in range(body * per_chunk, groups):
        rows = done[step * piece - body * chunk :][:piece]
        if step < regular - 1:
            keys[pl.ds(step * piece, piece), :] = rows
            key_copy(step).start()
        else:
            mask = peer_mask(me, step, groups, per_chunk)
            out_ref[pl.ds(pl.multiple_of(mask * piece, piece), piece), :] = rows

    def last_sent(s, carry):
        for j in range(1, parts):
            last_copy(j, s).wait_send()
        return carry

    lax.fori_loop(0, slices, last_sent, 0)
    early = [3 * (groups // 4) + i for i in range(per_chunk)]
    for step in range(regular - 1):
        key_wait(step, 0).wait_send()
    for mask in range(1, groups):
        if mask not in early:
            key_wait(0, mask).wait_recv()


def on_device(groups, parts, memory_rows, norm_gain, key_weight, owner_table):
    row_count, depth = memory_rows.shape
    columns = key_weight.shape[1]
    blocks = row_count // BLK_ROWS
    chunk = row_count // CHUNKS
    per_chunk = groups // CHUNKS
    slices = depth // min(SLICE, depth)
    any_space = pl.BlockSpec(memory_space=pl.ANY)
    in_hbm = pl.BlockSpec(memory_space=pltpu.HBM)
    in_vmem = pl.BlockSpec(memory_space=pltpu.VMEM)

    def kept(x):
        return pltpu.with_memory_space_constraint(x, pltpu.HBM)

    dma = pltpu.SemaphoreType.DMA
    incoming, slots = pl.pallas_call(
        functools.partial(main_kernel, groups, parts),
        out_shape=[
            jax.ShapeDtypeStruct((row_count, columns), jnp.bfloat16),
            jax.ShapeDtypeStruct((groups, blocks), jnp.int32),
        ],
        in_specs=[in_hbm, in_hbm, in_hbm, in_hbm],
        out_specs=[in_vmem, in_vmem],
        scratch_shapes=[
            pltpu.VMEM((groups, blocks), jnp.int32),
            pltpu.VMEM((groups, blocks), jnp.int32),
            pltpu.SMEM((groups, blocks), jnp.int32),
            pltpu.VMEM((blocks, BLK_ROWS, depth), jnp.bfloat16),
            pltpu.VMEM((blocks // CHUNKS, BLK_ROWS, depth), jnp.bfloat16),
            pltpu.VMEM((blocks, BLK_ROWS, depth), jnp.bfloat16),
            pltpu.VMEM((parts - 1, blocks, BLK_ROWS, depth), jnp.bfloat16),
            pltpu.VMEM((depth * parts, columns), jnp.bfloat16),
            pltpu.VMEM((row_count, columns), jnp.bfloat16),
            pltpu.VMEM((chunk, depth * parts), jnp.bfloat16),
            pltpu.VMEM((TAIL * chunk, depth * parts), jnp.bfloat16),
            pltpu.VMEM((1, depth * parts), jnp.float32),
            pltpu.VMEM((TAIL * chunk, columns), jnp.float32),
            pltpu.VMEM((LANES, LANES), jnp.float32),
            pltpu.VMEM((BLK_ROWS, LANES), jnp.float32),
            pltpu.VMEM((parts - 1, BLK_ROWS, LANES), jnp.float32),
            pltpu.VMEM((TAIL * chunk, LANES), jnp.float32),
            pltpu.VMEM((TAIL * chunk, LANES), jnp.float32),
            dma,
            dma,
            dma,
            dma((per_chunk,)),
            dma((per_chunk,)),
            dma((parts,)),
            dma,
            dma((parts - 1, CHUNKS)),
            dma((parts - 1, CHUNKS)),
            dma((parts - 1, slices)),
            dma((parts - 1, slices)),
            dma((parts - 1,)),
            dma((parts - 1,)),
            dma((groups,)),
            dma((groups,)),
            pltpu.SemaphoreType.REGULAR((4,)),
        ],
        compiler_params=pltpu.CompilerParams(
            collective_id=0, has_side_effects=True, vmem_limit_bytes=48 * MIB
        ),
        name="exchange",
    )(
        kept(owner_table.reshape(groups, blocks)),
        kept(memory_rows.reshape(blocks, BLK_ROWS, depth)),
        kept(norm_gain[None, :]),
        kept(key_weight),
    )

    placed = pl.pallas_call(
        functools.partial(place_kernel, groups),
        out_shape=jax.ShapeDtypeStruct((blocks, BLK_ROWS, columns), jnp.bfloat16),
        in_specs=[in_vmem, in_vmem],
        out_specs=any_space,
        scratch_shapes=[dma],
        compiler_params=pltpu.CompilerParams(vmem_limit_bytes=16 * MIB),
        name="place",
    )(slots, incoming.reshape(blocks, BLK_ROWS, columns))
    return placed.reshape(row_count, columns)


def solution(mesh):
    in_specs = (P("grp", "tp"), P(), P(None, "tp"), P())
    out_specs = P("grp", "tp")
    return jax.shard_map(
        functools.partial(on_device, mesh.shape["grp"], mesh.shape["tp"]),
        mesh=mesh, in_specs=in_specs, out_specs=out_specs, check_vma=False,
    )
```

```python
import functools

import jax
import jax.numpy as jnp
from jax import lax
from jax.experimental import pallas as pl
from jax.experimental.pallas import tpu as pltpu
from jax.sharding import PartitionSpec as P

BLK_ROWS = 8
EPS = 1e-05
CHUNKS = 16
LEAD = 4
SIDE = 4
TAIL = 2
STATS_AT = 4
HALF_AT = 9
SLICE = 128
LANES = 128
LOADS = 8
MIB = 1024 * 1024
MESH = pl.DeviceIdType.MESH


def flipped(me, mask, groups):
    out = me
    bit = 1
    while bit < groups:
        out = out + ((mask // bit) % 2) * bit * (1 - 2 * ((me // bit) % 2))
        bit *= 2
    return out


def peer_mask(me, step, groups, early):
    quarter = groups // 4
    half = quarter // 2
    one, two, three = ((far + 1) * quarter - 1 for far in (1, 2, 3))
    outer = ((one, quarter), (three, quarter - early), (two, quarter), (quarter - 1, quarter))
    inner = (
        (two, quarter), (quarter - 1, half), (three, quarter - early), (one, quarter), (half - 1, half)
    )

    def mask_in(runs):
        out = 0
        begin = 0
        for first, length in (*runs, (3 * quarter + early - 1, early)):
            out = jnp.where(step >= begin, first + begin - step, out)
            begin += length
        return out

    middle = ((me // quarter + 1) // 2) % 2
    return jnp.where(middle == 1, mask_in(inner), mask_in(outer))


def ranked(offset, value, capacity):
    groups, blocks = offset.shape
    lane = lax.broadcasted_iota(jnp.int32, (groups, blocks), 1)
    chosen = (offset >= 0) & (offset < blocks)
    counted = chosen.astype(jnp.int32)
    shift = 1
    while shift < blocks:
        counted = counted + jnp.where(lane >= shift, pltpu.roll(counted, shift, 1), 0)
        shift *= 2
    result = jnp.zeros((groups, blocks), jnp.int32)
    for r in range(capacity):
        at_rank = jnp.where(chosen & (counted == r + 1), value, 0).astype(jnp.float32)
        found = jnp.sum(at_rank, axis=1, keepdims=True).astype(jnp.int32)
        result = jnp.where(lane == r, found, result)
    return result


def place_kernel(groups, slot_ref, in_ref, out_ref, sem):
    me = lax.axis_index("grp")
    blocks = in_ref.shape[0]
    capacity = blocks // groups
    for mask in range(groups):
        slots = slot_ref[pl.ds(me ^ mask, 1), :]
        for r in range(capacity):
            pltpu.make_async_copy(
                in_ref.at[mask * capacity + r], out_ref.at[slots[0, r]], sem
            ).start()
    pltpu.make_async_copy(in_ref, out_ref, sem).wait()


def main_kernel(
    groups, parts, table_ref, rows_ref, gain_ref, weight_ref, out_ref, slot_ref,
    table, listed, index, raw, away, mine, others, weight, keys, normed, ready, gains, total,
    columns_stat, own_stat, peer_stat, means, scales,
    table_sem, index_sem, raw_sem, early_send, early_recv, weight_sem, gain_sem, gather_send, gather_recv,
    last_send, last_recv, stat_send, stat_recv, key_send, key_recv, met,
):
    me = lax.axis_index("grp")
    part = lax.axis_index("tp")
    blocks, _, depth = rows_ref.shape
    row_count = blocks * BLK_ROWS
    width = depth * parts
    chunk = row_count // CHUNKS
    chunk_blocks = blocks // CHUNKS
    capacity = blocks // groups
    per_chunk = groups // CHUNKS
    piece = row_count // groups
    regular = groups - per_chunk
    last = CHUNKS - 1
    body = CHUNKS - TAIL
    tail = TAIL * chunk
    tail_blocks = TAIL * chunk_blocks
    slice_width = min(SLICE, depth)
    slices = depth // slice_width
    sub = 2 * BLK_ROWS

    table_copy = pltpu.make_async_copy(table_ref, table, table_sem)
    table_copy.start()
    line = me // SIDE
    lines = groups // SIDE
    loads = min(LOADS, blocks)
    for i in range(loads):
        at = pl.ds(i * (blocks // loads), blocks // loads)
        pltpu.make_async_copy(rows_ref.at[at], raw.at[at], raw_sem).start()
    gain_copy = pltpu.make_async_copy(gain_ref, gains, gain_sem)
    gain_copy.start()

    barrier = pltpu.get_barrier_semaphore()

    def greet(sem, device):
        pl.semaphore_signal(sem, inc=1, device_id=device, device_id_type=MESH)

    for j in range(1, parts):
        greet(barrier, {"tp": (part + j) % parts})
    for bit in range(2):
        greet(barrier, {"grp": flipped(me, 1 << bit, SIDE)})

    @pl.when(line > 0)
    def _():
        greet(barrier, {"grp": me - SIDE})

    @pl.when(line < lines - 1)
    def _():
        greet(barrier, {"grp": me + SIDE})

    def weight_copy(j):
        origin = (part + j) % parts
        return pltpu.make_async_copy(
            weight_ref.at[pl.ds(pl.multiple_of(origin * depth, depth), depth)],
            weight.at[pl.ds(j * depth, depth)],
            weight_sem.at[j],
        )

    def gain_at(j, first, count):
        origin = (part + j) % parts
        return gains[:, pl.ds(pl.multiple_of(origin * depth + first, LANES), count)]

    def gather_copy(c, j):
        at = pl.ds(c * chunk_blocks, chunk_blocks)
        return pltpu.make_async_remote_copy(
            src_ref=mine.at[at],
            dst_ref=others.at[j - 1, at],
            send_sem=gather_send.at[j - 1, c],
            recv_sem=gather_recv.at[j - 1, c],
            device_id={"tp": (part + parts - j) % parts},
            device_id_type=MESH,
        )

    def last_copy(j, s):
        at = pl.ds(body * chunk_blocks, tail_blocks)
        cols = pl.ds(pl.multiple_of(s * slice_width, slice_width), slice_width)
        return pltpu.make_async_remote_copy(
            src_ref=mine.at[at, :, cols],
            dst_ref=others.at[j - 1, at, :, cols],
            send_sem=last_send.at[j - 1, s],
            recv_sem=last_recv.at[j - 1, s],
            device_id={"tp": (part + parts - j) % parts},
            device_id_type=MESH,
        )

    def stat_copy(j):
        return pltpu.make_async_remote_copy(
            src_ref=own_stat,
            dst_ref=peer_stat.at[j - 1],
            send_sem=stat_send.at[j - 1],
            recv_sem=stat_recv.at[j - 1],
            device_id={"tp": (part + parts - j) % parts},
            device_id_type=MESH,
        )

    def key_copy(step):
        mask = peer_mask(me, step, groups, per_chunk)
        return pltpu.make_async_remote_copy(
            src_ref=keys.at[pl.ds(step * piece, piece)],
            dst_ref=out_ref.at[pl.ds(mask * piece, piece)],
            send_sem=key_send.at[step],
            recv_sem=key_recv.at[mask],
            device_id={"grp": flipped(me, mask, groups)},
            device_id_type=MESH,
        )

    def key_wait(step, mask):
        return pltpu.make_async_remote_copy(
            src_ref=keys.at[pl.ds(step * piece, piece)],
            dst_ref=out_ref.at[pl.ds(mask * piece, piece)],
            send_sem=key_send.at[step],
            recv_sem=key_recv.at[mask],
            device_id={"grp": flipped(me, 1, SIDE)},
            device_id_type=MESH,
        )

    def early_copy(i):
        mask = peer_mask(me, regular + i, groups, per_chunk)
        return pltpu.make_async_remote_copy(
            src_ref=away.at[pl.ds(i * capacity, capacity)],
            dst_ref=mine.at[pl.ds((regular + i) * capacity, capacity)],
            send_sem=early_send.at[i],
            recv_sem=early_recv.at[i],
            device_id={"grp": flipped(me, mask, groups)},
            device_id_type=MESH,
        )

    def arrange(c):
        def take(i, carry):
            step = i // capacity
            at = index[step, i - step * capacity]
            block = raw[jnp.minimum(jnp.maximum(at, 0), blocks - 1)]
            if c == last:
                away[i - c * chunk_blocks] = block
            else:
                mine[i] = block
            return carry

        lax.fori_loop(c * chunk_blocks, (c + 1) * chunk_blocks, take, 0, unroll=2)

    row = lax.broadcasted_iota(jnp.int32, (groups, blocks), 0)
    lane = lax.broadcasted_iota(jnp.int32, (groups, blocks), 1)
    peer = jnp.zeros((groups, blocks), jnp.int32)
    for step in range(groups):
        mask = peer_mask(me, step, groups, per_chunk)
        peer = jnp.where(row == step, flipped(me, mask, groups), peer)
    table_copy.wait()
    own = jnp.broadcast_to(table[pl.ds(me, 1), :], (groups, blocks))
    listed[...] = ranked(own - peer * blocks, lane, capacity)
    index_copy = pltpu.make_async_copy(listed, index, index_sem)
    index_copy.start()
    pltpu.make_async_copy(rows_ref, raw, raw_sem).wait()
    for j in range(parts):
        weight_copy(j).start()

    for i in range(chunk_blocks):
        at = listed[pl.ds(i // capacity, 1), pl.ds(i % capacity, 1)][0, 0]
        mine[i] = raw[jnp.minimum(jnp.maximum(at, 0), blocks - 1)]
    inner = (line > 0) & (line < lines - 1)
    neighbours = 1 + inner.astype(jnp.int32)
    pl.semaphore_wait(barrier, parts - 1 + 2 + neighbours)

    def gather(c):
        for j in range(1, parts):
            gather_copy(c, j).start()

    def send_early():
        for i in range(per_chunk):
            early_copy(i).start()

    gather(0)
    index_copy.wait()
    arrange(last)
    near = lines == 4 and per_chunk == 1
    if near:

        @pl.when(inner)
        def _():
            send_early()

    arrange(1)
    gather(1)

    def from_below():
        @pl.when(line > 1)
        def _():
            pl.semaphore_wait(met.at[0], 1)

        @pl.when((line > 0) & (line < lines - 1))
        def _():
            greet(met.at[0], {"grp": me + SIDE})

    def from_above():
        @pl.when(line < lines - 2)
        def _():
            pl.semaphore_wait(met.at[1], 1)

        @pl.when((line > 0) & (line < lines - 1))
        def _():
            greet(met.at[1], {"grp": me - SIDE})

    @pl.when(line < lines // 2)
    def _():
        from_below()
        from_above()

    @pl.when(line >= lines // 2)
    def _():
        from_above()
        from_below()

    if near:

        @pl.when(jnp.logical_not(inner))
        def _():
            send_early()

    for bit in range(2):
        greet(met.at[2 + bit], {"grp": flipped(me, 1 << bit, SIDE)})
        pl.semaphore_wait(met.at[2 + bit], 1)
    if not near:
        send_early()
    for c in range(2, last):
        arrange(c)
        if c < LEAD:
            gather(c)

    offset = table[...] - me * blocks
    slot_ref[...] = ranked(offset, offset, capacity)
    columns_stat[...] = jnp.zeros_like(columns_stat)
    gain_copy.wait()
    for j in range(parts):
        weight_copy(j).wait()

    def stored(c, i, j, first, count):
        at = pl.ds(c * chunk_blocks + i * 2, 2)
        cols = pl.ds(first, count)
        held = mine[at, :, cols] if j == 0 else others[j - 1, at, :, cols]
        return held.astype(jnp.float32).reshape(sub, count)

    def rows_at(i):
        return pl.ds(pl.multiple_of(i * sub, sub), sub)

    def own_sums():
        def sums(i, carry):
            x = stored(body, i, 0, 0, depth)
            row_sum = jnp.sum(x, axis=1, keepdims=True)
            row_sq = jnp.sum(x * x, axis=1, keepdims=True)
            where = lax.broadcasted_iota(jnp.int32, (sub, LANES), 1)
            columns_stat[rows_at(i), :] = jnp.where(
                where == 0, row_sum, jnp.where(where == 1, row_sq, 0.0)
            )
            return carry

        lax.fori_loop(0, tail // sub, sums, 0)
        own_stat[...] = jnp.transpose(columns_stat[...])[:BLK_ROWS]

    def all_sums():
        sums = own_stat[...]
        for j in range(1, parts):
            sums = sums + peer_stat[j - 1]
        columns_stat[:BLK_ROWS, :] = sums
        columns = jnp.transpose(columns_stat[...])[:tail]
        mean = columns[:, 0:1] / width
        means[...] = jnp.broadcast_to(mean, means.shape)
        scale = lax.rsqrt(columns[:, 1:2] / width - mean * mean + EPS)
        scales[...] = jnp.broadcast_to(scale, scales.shape)

    def last_norm(j, first, count):
        def norm_rows(i, carry):
            for k in range(count // LANES):
                at = pl.multiple_of(first + k * LANES, LANES)
                x = stored(body, i, j, at, LANES)
                ready[rows_at(i), pl.ds(pl.multiple_of(j * depth + at, LANES), LANES)] = (
                    (x - means[rows_at(i), :]) * scales[rows_at(i), :] * gain_at(j, at, LANES)
                ).astype(jnp.bfloat16)
            return carry

        lax.fori_loop(0, tail // sub, norm_rows, 0, unroll=count <= SLICE)

    def last_product(j, first, count):
        at = pl.ds(pl.multiple_of(j * depth + first, LANES), count)
        return jnp.dot(ready[:, at], weight[at, :], preferred_element_type=jnp.float32)

    def one_chunk(c, carry):
        base = pl.multiple_of(c * chunk, chunk)

        @pl.when(c == STATS_AT)
        def _():
            for i in range(per_chunk):
                early_copy(i).wait_recv()
            own_sums()
            for j in range(1, parts):
                stat_copy(j).start()

        @pl.when(c == HALF_AT)
        def _():
            for j in range(1, parts):
                stat_copy(j).wait_recv()
            all_sums()
            last_norm(0, 0, depth)
            total[...] = last_product(0, 0, depth)

        for j in range(1, parts):
            gather_copy(c, j).wait_recv()

        @pl.when(c + LEAD < body)
        def _():
            for j in range(1, parts):
                gather_copy(c + LEAD, j).start()

        @pl.when(c + LEAD == body)
        def _():
            def send(s, carry):
                for j in range(1, parts):
                    last_copy(j, s).start()
                return carry

            lax.fori_loop(0, slices, send, 0)

        def norm_rows(i, carry):
            row_sum = 0.0
            row_sq = 0.0
            for j in range(parts):
                x = stored(c, i, j, 0, depth)
                row_sum = row_sum + jnp.sum(x, axis=1, keepdims=True)
                row_sq = row_sq + jnp.sum(x * x, axis=1, keepdims=True)
            mean = row_sum / width
            scale = lax.rsqrt(row_sq / width - mean * mean + EPS)
            for j in range(parts):
                normed[rows_at(i), pl.ds(j * depth, depth)] = (
                    (stored(c, i, j, 0, depth) - mean) * scale * gain_at(j, 0, depth)
                ).astype(jnp.bfloat16)
            return carry

        lax.fori_loop(0, chunk // sub, norm_rows, 0)
        keys[pl.ds(base, chunk), :] = jnp.dot(
            normed[...], weight[...], preferred_element_type=jnp.float32
        ).astype(jnp.bfloat16)

        for i in range(per_chunk):
            key_copy(c * per_chunk + i).start()

        return carry

    lax.fori_loop(0, body, one_chunk, 0)

    for i in range(per_chunk):
        early_copy(i).wait_send()
    for j in range(1, parts):
        stat_copy(j).wait_send()

    def sent(c, carry):
        for j in range(1, parts):
            gather_copy(c, j).wait_send()
        return carry

    lax.fori_loop(0, body, sent, 0)

    def last_slice(s, j):
        first = s * slice_width
        last_copy(j, s).wait_recv()
        last_norm(j, first, slice_width)
        return last_product(j, first, slice_width)

    def add_slice(s, carry):
        for j in range(1, parts):
            total[...] += last_slice(s, j)
        return carry

    lax.fori_loop(0, slices - 1, add_slice, 0)
    for j in range(1, parts - 1):
        total[...] += last_slice(slices - 1, j)
    done = (total[...] + last_slice(slices - 1, parts - 1)).astype(jnp.bfloat16)
    for step in range(body * per_chunk, groups):
        rows = done[step * piece - body * chunk :][:piece]
        if step < regular - 1:
            keys[pl.ds(step * piece, piece), :] = rows
            key_copy(step).start()
        else:
            mask = peer_mask(me, step, groups, per_chunk)
            out_ref[pl.ds(pl.multiple_of(mask * piece, piece), piece), :] = rows

    def last_sent(s, carry):
        for j in range(1, parts):
            last_copy(j, s).wait_send()
        return carry

    lax.fori_loop(0, slices, last_sent, 0)
    early = [3 * (groups // 4) + i for i in range(per_chunk)]
    for step in range(regular - 1):
        key_wait(step, 0).wait_send()
    for mask in range(1, groups):
        if mask not in early:
            key_wait(0, mask).wait_recv()


def on_device(groups, parts, memory_rows, norm_gain, key_weight, owner_table):
    row_count, depth = memory_rows.shape
    columns = key_weight.shape[1]
    blocks = row_count // BLK_ROWS
    chunk = row_count // CHUNKS
    per_chunk = groups // CHUNKS
    slices = depth // min(SLICE, depth)
    any_space = pl.BlockSpec(memory_space=pl.ANY)
    in_hbm = pl.BlockSpec(memory_space=pltpu.HBM)
    in_vmem = pl.BlockSpec(memory_space=pltpu.VMEM)

    def kept(x):
        return pltpu.with_memory_space_constraint(x, pltpu.HBM)

    dma = pltpu.SemaphoreType.DMA
    incoming, slots = pl.pallas_call(
        functools.partial(main_kernel, groups, parts),
        out_shape=[
            jax.ShapeDtypeStruct((row_count, columns), jnp.bfloat16),
            jax.ShapeDtypeStruct((groups, blocks), jnp.int32),
        ],
        in_specs=[in_hbm, in_hbm, in_hbm, in_hbm],
        out_specs=[in_vmem, in_vmem],
        scratch_shapes=[
            pltpu.VMEM((groups, blocks), jnp.int32),
            pltpu.VMEM((groups, blocks), jnp.int32),
            pltpu.SMEM((groups, blocks), jnp.int32),
            pltpu.VMEM((blocks, BLK_ROWS, depth), jnp.bfloat16),
            pltpu.VMEM((blocks // CHUNKS, BLK_ROWS, depth), jnp.bfloat16),
            pltpu.VMEM((blocks, BLK_ROWS, depth), jnp.bfloat16),
            pltpu.VMEM((parts - 1, blocks, BLK_ROWS, depth), jnp.bfloat16),
            pltpu.VMEM((depth * parts, columns), jnp.bfloat16),
            pltpu.VMEM((row_count, columns), jnp.bfloat16),
            pltpu.VMEM((chunk, depth * parts), jnp.bfloat16),
            pltpu.VMEM((TAIL * chunk, depth * parts), jnp.bfloat16),
            pltpu.VMEM((1, depth * parts), jnp.float32),
            pltpu.VMEM((TAIL * chunk, columns), jnp.float32),
            pltpu.VMEM((LANES, LANES), jnp.float32),
            pltpu.VMEM((BLK_ROWS, LANES), jnp.float32),
            pltpu.VMEM((parts - 1, BLK_ROWS, LANES), jnp.float32),
            pltpu.VMEM((TAIL * chunk, LANES), jnp.float32),
            pltpu.VMEM((TAIL * chunk, LANES), jnp.float32),
            dma,
            dma,
            dma,
            dma((per_chunk,)),
            dma((per_chunk,)),
            dma((parts,)),
            dma,
            dma((parts - 1, CHUNKS)),
            dma((parts - 1, CHUNKS)),
            dma((parts - 1, slices)),
            dma((parts - 1, slices)),
            dma((parts - 1,)),
            dma((parts - 1,)),
            dma((groups,)),
            dma((groups,)),
            pltpu.SemaphoreType.REGULAR((4,)),
        ],
        compiler_params=pltpu.CompilerParams(
            collective_id=0, has_side_effects=True, vmem_limit_bytes=48 * MIB
        ),
        name="exchange",
    )(
        kept(owner_table.reshape(groups, blocks)),
        kept(memory_rows.reshape(blocks, BLK_ROWS, depth)),
        kept(norm_gain[None, :]),
        kept(key_weight),
    )

    placed = pl.pallas_call(
        functools.partial(place_kernel, groups),
        out_shape=jax.ShapeDtypeStruct((blocks, BLK_ROWS, columns), jnp.bfloat16),
        in_specs=[in_vmem, in_vmem],
        out_specs=any_space,
        scratch_shapes=[dma],
        compiler_params=pltpu.CompilerParams(vmem_limit_bytes=16 * MIB),
        name="place",
    )(slots, incoming.reshape(blocks, BLK_ROWS, columns))
    return placed.reshape(row_count, columns)


def solution(mesh):
    in_specs = (P("grp", "tp"), P(), P(None, "tp"), P())
    out_specs = P("grp", "tp")
    return jax.shard_map(
        functools.partial(on_device, mesh.shape["grp"], mesh.shape["tp"]),
        mesh=mesh, in_specs=in_specs, out_specs=out_specs, check_vma=False,
    )
```
